32 devices in a mesh: dst: 8 (over z, core), src: 4 (over y, x).
Axes of the slice: x: 2, y: 2, z: 4, core: 2. Of those that a mesh axis runs over, the one named last changes fastest.
Arguments:
- features: bfloat16 [256, 3712], P(('dst', 'src')), may hold values from -6 to 6
- edge_source: int32 [8, 2048], P('dst', 'src'), may hold values from 0 to 255, as said below
- edge_target: int32 [8, 2048], P('dst', 'src'), may hold values from 0 to 255, as said below
- edge_valid: int32 [8, 2048], P('dst', 'src'), may hold values from 0 to 1, as said below
- edge_radial: bfloat16 [8, 2048, 128], P('dst', 'src'), may hold values from -6 to 6
- edge_bias: float32 [8, 8, 2048], P('dst', None, 'src'), may hold values from -10 to 330
- w_radial: bfloat16 [128, 128], replicated, may hold values from -0.5 to 0.5
- w_zero: bfloat16 [896, 896], replicated, may hold values from -0.1875 to 0.1875
- w_one_re: bfloat16 [768, 768], replicated, may hold values from -0.15625 to 0.15625
- w_one_im: bfloat16 [768, 768], replicated, may hold values from -0.15625 to 0.15625
- w_two_re: bfloat16 [640, 640], replicated, may hold values from -0.15625 to 0.15625
- w_two_im: bfloat16 [640, 640], replicated, may hold values from -0.15625 to 0.15625
- att_vector: float32 [128], replicated, may hold values from -3 to 3
- w_out: bfloat16 [7, 128, 128], replicated, may hold values from -0.5 to 0.5
Outputs:
- attended: bfloat16 [256, 3712], P(('dst', 'src'))
The draws below stay inside these ranges and needn't reach their ends.
Inputs may be any that keep to these rules, and one draw needn't show every extreme that they name: `edge_source`: in row d, column block s (the tile of destination block d and source block s) every entry is an atom a with (a // 8) % 4 == s. `edge_target`: in row d every entry lies in [d * 8 * 4, (d + 1) * 8 * 4); every atom is the target of at least one valid slot. `edge_valid`: about five sixteenths of the slots are valid.
All inputs are finite; a program needn't handle non-finite values.
Results may differ from the reference program's by a relative error of at most 0.0093.
Values may be sent and summed in bfloat16 or wider, within the bound.
A program may use at most 128 MiB of HBM per device.

```python
import jax
import jax.numpy as jnp
import numpy as np
from jax import lax

C = 128
HEADS = 8
LMAX = 6
NCOEF = 29
RAD = 128
A_DEV = 8
DST_BLOCKS = 8
SRC_BLOCKS = 4
ATOMS = 256
ECAP = 512


def edge_layout(key):
    shape = (DST_BLOCKS, SRC_BLOCKS, ECAP)
    dst_atoms = A_DEV * SRC_BLOCKS
    src_atoms = A_DEV * DST_BLOCKS
    target_local = jax.random.randint(jax.random.fold_in(key, 11), shape, 0, dst_atoms)
    source_local = jax.random.randint(jax.random.fold_in(key, 12), shape, 0, src_atoms)
    valid = (jax.random.randint(jax.random.fold_in(key, 13), shape, 0, 16) < 5).astype(jnp.int32)
    slot = lax.broadcasted_iota(jnp.int32, shape, 2)
    block_src = lax.broadcasted_iota(jnp.int32, shape, 1)
    block_dst = lax.broadcasted_iota(jnp.int32, shape, 0)
    forced = slot < A_DEV
    target_local = jnp.where(forced, block_src * A_DEV + slot, target_local)
    valid = jnp.where(forced, 1, valid)
    source = source_local // A_DEV * (A_DEV * SRC_BLOCKS) + block_src * A_DEV + source_local % A_DEV
    target = block_dst * dst_atoms + target_local
    return (source.reshape(DST_BLOCKS, SRC_BLOCKS * ECAP).astype(jnp.int32), target.reshape(DST_BLOCKS, SRC_BLOCKS * ECAP).astype(jnp.int32), valid.reshape(DST_BLOCKS, SRC_BLOCKS * ECAP).astype(jnp.int32))


def draw_edge_source(key, part):
    return edge_layout(key)[0]


def draw_edge_target(key, part):
    return edge_layout(key)[1]


def draw_edge_valid(key, part):
    return edge_layout(key)[2]


def draw_edge_bias(key, part):
    shape = (DST_BLOCKS, HEADS, SRC_BLOCKS * ECAP)
    noise = jax.random.normal(jax.random.fold_in(key, 21), shape, jnp.float32)
    return jnp.clip(noise, -4.0, 4.0)


def level_of(stream_key, shape, pieces, smallest, largest):
    factor_of, own = 1.0, jax.random.fold_in(stream_key, 6)
    for axis_at, shards_of in pieces:
        steps = jnp.exp(jax.random.uniform(jax.random.fold_in(own, axis_at), (shards_of,), jnp.float32, smallest / len(pieces), largest / len(pieces)))
        factor_of = factor_of * jnp.repeat(steps, shape[axis_at] // shards_of).reshape([-1 if axis == axis_at else 1 for axis in range(len(shape))])
    return factor_of


def gaussian(rng, extent, spread, bound, split=(), kind=jnp.bfloat16):
    entries = jax.random.normal(rng, extent, jnp.float32) * spread
    if len(split) > 0:
        entries = level_of(rng, extent, split, -0.22, 0.18) * entries
    return jnp.clip(entries, min=-bound, max=bound).astype(kind)


def setup_inputs(seed: int = 0) -> dict:
    key_list = jax.random.split(jax.random.key(seed), 15)
    return {
        "features": gaussian(key_list[0], (ATOMS, NCOEF * C), 1.0, 6.0, ((0, 32),)),
        "edge_source": draw_edge_source(jax.random.fold_in(key_list[14], 71), 0),
        "edge_target": draw_edge_target(jax.random.fold_in(key_list[14], 71), 0),
        "edge_valid": draw_edge_valid(jax.random.fold_in(key_list[14], 71), 0),
        "edge_radial": gaussian(key_list[4], (DST_BLOCKS, SRC_BLOCKS * ECAP, RAD), 1.0, 6.0, ((0, 8), (1, 4))),
        "edge_bias": draw_edge_bias(jax.random.fold_in(key_list[14], 71), 0),
        "w_radial": gaussian(key_list[6], (RAD, C), RAD ** -0.5, 0.5),
        "w_zero": gaussian(key_list[7], (7 * C, 7 * C), (7 * C) ** -0.5, 0.1875),
        "w_one_re": gaussian(key_list[8], (6 * C, 6 * C), (12 * C) ** -0.5, 0.15625),
        "w_one_im": gaussian(key_list[9], (6 * C, 6 * C), (12 * C) ** -0.5, 0.15625),
        "w_two_re": gaussian(key_list[10], (5 * C, 5 * C), (10 * C) ** -0.5, 0.15625),
        "w_two_im": gaussian(key_list[11], (5 * C, 5 * C), (10 * C) ** -0.5, 0.15625),
        "att_vector": gaussian(key_list[12], (C,), 0.5, 3.0, (), jnp.float32),
        "w_out": gaussian(key_list[13], (LMAX + 1, C, C), C ** -0.5, 0.5),
    }


NEG = -1e30


def product(left, right):
    return jnp.dot(left.astype(jnp.float32), right.astype(jnp.float32), preferred_element_type=jnp.float32)


def spread_heads(weights, copies, channels):
    return jnp.tile(jnp.repeat(weights, channels // weights.shape[1], axis=1), (1, copies))


def degree_table():
    return np.array(list(range(7)) + list(range(1, 7)) * 2 + list(range(2, 7)) * 2, dtype=np.int32)


def edge_messages(rows, gain, w_zero, w_one_re, w_one_im, w_two_re, w_two_im, att_vector):
    channels = gain.shape[1]
    count = rows.shape[0]

    def part(low, high):
        return (rows[:, low * channels:high * channels].astype(jnp.float32) * jnp.tile(gain, (1, high - low))).astype(jnp.bfloat16)

    zero = part(0, 7)
    up_one, uq_one = part(7, 13), part(13, 19)
    up_two, uq_two = part(19, 24), part(24, 29)
    out_zero = product(zero, w_zero)
    yp_one = product(up_one, w_one_re) - product(uq_one, w_one_im)
    yq_one = product(up_one, w_one_im) + product(uq_one, w_one_re)
    yp_two = product(up_two, w_two_re) - product(uq_two, w_two_im)
    yq_two = product(up_two, w_two_im) + product(uq_two, w_two_re)
    active = jax.nn.silu(out_zero[:, :channels]) * att_vector[None, :]
    logit = active.reshape(count, HEADS, channels // HEADS).sum(axis=2)
    values = jnp.concatenate([out_zero, yp_one, yq_one, yp_two, yq_two], axis=1)
    return logit, values


def reference(features, edge_source, edge_target, edge_valid, edge_radial, edge_bias, w_radial, w_zero, w_one_re, w_one_im, w_two_re, w_two_im, att_vector, w_out):
    dst_atoms = A_DEV * SRC_BLOCKS
    selected = w_out[degree_table()]

    def one_block(items):
        source, target, valid_int, radial, bias, block = items
        valid = valid_int > 0
        rows = features[source]
        gain = product(radial, w_radial)
        logit, values = edge_messages(rows, gain, w_zero, w_one_re, w_one_im, w_two_re, w_two_im, att_vector)
        logit = logit + bias.T
        local_target = (target - block * dst_atoms).astype(jnp.int32)
        masked = jnp.where(valid[:, None], logit, NEG)
        top = jnp.maximum(jax.ops.segment_max(masked, local_target, num_segments=dst_atoms), NEG)
        shifted = jnp.where(valid[:, None], logit - top[local_target], 0.0)
        weights = jnp.where(valid[:, None], jnp.exp(shifted), 0.0)
        den = jax.ops.segment_sum(weights, local_target, num_segments=dst_atoms)
        num = jax.ops.segment_sum(values * spread_heads(weights, NCOEF, C), local_target, num_segments=dst_atoms)
        merged = (num / spread_heads(den, NCOEF, C)).astype(jnp.bfloat16)
        shaped = merged.reshape(dst_atoms, NCOEF, C).astype(jnp.float32)
        projected = jnp.einsum("acx,cxy->acy", shaped, selected.astype(jnp.float32))
        return projected.astype(jnp.bfloat16).reshape(dst_atoms, NCOEF * C)

    blocks = jnp.arange(DST_BLOCKS, dtype=jnp.int32)
    result = lax.map(one_block, (edge_source, edge_target, edge_valid, edge_radial, edge_bias, blocks))
    return result.reshape(ATOMS, NCOEF * C)
```

```python
import functools

import jax
import jax.numpy as jnp
from jax import lax
from jax.experimental import pallas as pl
from jax.experimental.pallas import tpu as pltpu
from jax.sharding import PartitionSpec as P

HEADS = 8
NEG = -1e30
MESH = pl.DeviceIdType.MESH
CORES = 2
PIECES = ((0, 7), (7, 12), (19, 10))
DEGREES = list(range(7)) + list(range(1, 7)) * 2 + list(range(2, 7)) * 2
F32 = jnp.float32
BF16 = jnp.bfloat16


def dot(left, right):
    return jnp.dot(left, right, preferred_element_type=F32)


def kernel(
    n_dst,
    n_src,
    feat_ref,
    source_ref,
    target_ref,
    valid_ref,
    radial_ref,
    bias_ref,
    w_radial_ref,
    att_ref,
    w_zero_hbm,
    w_one_re_hbm,
    w_one_im_hbm,
    w_two_re_hbm,
    w_two_im_hbm,
    w_out_hbm,
    out_ref,
    w_zero,
    w_one_re,
    w_one_im,
    w_two_re,
    w_two_im,
    w_out,
    feat_buf,
    feat_all,
    gain_ref,
    onehot_ref,
    u_ref,
    weight_ref,
    num_ref,
    send_num,
    recv_num,
    send_stat,
    recv_stat,
    merged_ref,
    load_sem,
    z_send,
    pair_send,
    feat_recv,
    num_send,
    num_recv,
):
    own = feat_ref.shape[0]
    channels = w_radial_ref.shape[1]
    slots = source_ref.shape[1]
    block = own * n_src
    atoms = own * n_dst
    nz = n_dst // CORES
    per_head = channels // HEADS
    d = lax.axis_index("dst")
    s = lax.axis_index("src")
    z = d // CORES
    core = d % CORES
    partner = d + 1 - 2 * core

    def line(j):
        return lax.rem(z + j, nz) * CORES + core

    def other(j):
        return lax.rem(s + j, n_src)

    barrier = pltpu.get_barrier_semaphore()
    for j in range(1, nz):
        pl.semaphore_signal(barrier, inc=1, device_id=(line(j), s), device_id_type=MESH)
    for j in range(1, n_src):
        pl.semaphore_signal(barrier, inc=1, device_id=(d, other(j)), device_id_type=MESH)
    pl.semaphore_signal(barrier, inc=1, device_id=(partner, s), device_id_type=MESH)

    loads = [
        pltpu.make_async_copy(src, dst, load_sem.at[i])
        for i, (src, dst) in enumerate(
            (
                (w_zero_hbm, w_zero),
                (w_one_re_hbm, w_one_re),
                (w_one_im_hbm, w_one_im),
                (w_two_re_hbm, w_two_re),
                (w_two_im_hbm, w_two_im),
                (w_out_hbm, w_out),
            )
        )
    ]
    for load in loads:
        load.start()

    def span(k):
        first, count = PIECES[k]
        return pl.ds(first * channels, count * channels)

    def feature_copy(k, src, index, send, target):
        return pltpu.make_async_remote_copy(
            src_ref=src,
            dst_ref=feat_buf.at[index, :, span(k)],
            send_sem=send,
            recv_sem=feat_recv.at[index, k],
            device_id=(target, s),
            device_id_type=MESH,
        )

    pl.semaphore_wait(barrier, nz - 1 + n_src - 1 + 1)

    started = []
    for k in range(len(PIECES)):
        mine = feat_ref.at[:, span(k)]
        for j in range(1, nz):
            copy = feature_copy(k, mine, d, z_send.at[j, k], line(j))
            copy.start()
            started.append(copy)
        copy = feature_copy(k, mine, d, pair_send.at[0, k], partner)
        copy.start()
        started.append(copy)

    gain_ref[...] = dot(radial_ref[0], w_radial_ref[...])
    source = source_ref[...]
    row = source // block * own + source % own
    picks = lax.broadcasted_iota(jnp.int32, (atoms, slots), 0) == row
    onehot_ref[...] = jnp.transpose(picks.astype(F32)).astype(BF16)

    def relay(k):
        for j in range(1, nz):
            index = line(j)
            feature_copy(k, feat_buf.at[index, :, span(k)], index, z_send.at[j, k], index).wait_recv()
            copy = feature_copy(k, feat_buf.at[index, :, span(k)], index, pair_send.at[j, k], partner)
            copy.start()
            started.append(copy)

    def collect(k):
        mine = pl.ds(pl.multiple_of(d * own, own), own)
        feat_all[mine, span(k)] = feat_ref[:, span(k)].astype(F32)
        for j in range(1, nz):
            index = line(j)
            rows = pl.ds(pl.multiple_of(index * own, own), own)
            feat_all[rows, span(k)] = feat_buf[index, :, span(k)].astype(F32)
        for j in range(nz):
            index = lax.rem(z + j, nz) * CORES + 1 - core
            feature_copy(k, feat_buf.at[index, :, span(k)], index, pair_send.at[j, k], partner).wait_recv()
            rows = pl.ds(pl.multiple_of(index * own, own), own)
            feat_all[rows, span(k)] = feat_buf[index, :, span(k)].astype(F32)

    def spread(k):
        first, count = PIECES[k]
        rows = dot(onehot_ref[...], feat_all[:, span(k)].astype(BF16))
        gain = gain_ref[...]
        for i in range(count):
            at = (first + i) * channels
            u_ref[:, at : at + channels] = (rows[:, i * channels : (i + 1) * channels] * gain).astype(BF16)

    head_of = lax.broadcasted_iota(jnp.int32, (1, channels), 1) // per_head
    together = max(1, 256 // block)
    groups = HEADS // together

    def gather_sums(k, group):
        first, count = PIECES[k]
        rows = pl.ds(group * (together * block), together * block)
        weights = weight_ref[rows, :]
        sums = dot(weights, u_ref[:, span(k)]).astype(BF16)
        if k == 0:
            parts = [dot(sums, w_zero[...])]
        else:
            w_re, w_im = ((w_one_re, w_one_im), (w_two_re, w_two_im))[k - 1]
            half = count // 2 * channels
            plus, minus = sums[:, :half], sums[:, half:]
            parts = [
                dot(plus, w_re[...]) - dot(minus, w_im[...]),
                dot(plus, w_im[...]) + dot(minus, w_re[...]),
            ]
        at = first
        for part in parts:
            for i in range(part.shape[1] // channels):
                columns = pl.ds(at * channels, channels)
                at += 1
                value = part[:, i * channels : (i + 1) * channels]
                total = num_ref[:, columns] if groups > 1 else jnp.zeros((block, channels), F32)
                for j in range(together):
                    head = group * together + j
                    total = jnp.where(head_of == head, value[j * block : (j + 1) * block], total)
                num_ref[:, columns] = total

    def sums_of(k):
        if groups == 1:
            gather_sums(k, 0)
        else:
            lax.fori_loop(0, groups, lambda g, c: (gather_sums(k, g), c)[1], 0)
        first, count = PIECES[k]
        for p in range(n_src):
            send_num[p, :, span(k)] = num_ref[p * own : (p + 1) * own, span(k)].astype(BF16)

    def stat_copy(j, source_at):
        return pltpu.make_async_remote_copy(
            src_ref=send_stat.at[other(j)],
            dst_ref=recv_stat.at[source_at],
            send_sem=num_send.at[j, len(PIECES)],
            recv_sem=num_recv.at[source_at, len(PIECES)],
            device_id=(d, other(j)),
            device_id_type=MESH,
        )

    def num_copy(j, k, source_at):
        return pltpu.make_async_remote_copy(
            src_ref=send_num.at[other(j), :, span(k)],
            dst_ref=recv_num.at[source_at, :, span(k)],
            send_sem=num_send.at[j, k],
            recv_sem=num_recv.at[source_at, k],
            device_id=(d, other(j)),
            device_id_type=MESH,
        )

    def send_sums(k):
        for j in range(1, n_src):
            copy = num_copy(j, k, s)
            copy.start()
            started.append(copy)

    relay(0)
    collect(0)
    spread(0)
    loads[0].wait()
    scalar = dot(u_ref[:, span(0)], w_zero[:, :channels])
    active = scalar / (1.0 + jnp.exp(-scalar))
    att = jnp.where(
        lax.broadcasted_iota(jnp.int32, (HEADS, channels), 0) == head_of, att_ref[...], 0.0
    )
    logit = lax.dot_general(
        att,
        active,
        (((1,), (1,)), ((), ())),
        precision=lax.Precision.HIGHEST,
        preferred_element_type=F32,
    ) + bias_ref[0]
    local_target = target_ref[...] - d * block
    member = (lax.broadcasted_iota(jnp.int32, (block, slots), 0) == local_target) & (valid_ref[...] > 0)
    tops = jnp.zeros((block, channels), F32)
    dens = jnp.zeros((block, channels), F32)
    for h in range(HEADS):
        masked = jnp.where(member, logit[h : h + 1, :], NEG)
        top = jnp.max(masked, axis=1, keepdims=True)
        weight = jnp.where(member, jnp.exp(masked - top), 0.0).astype(BF16)
        weight_ref[h * block : (h + 1) * block, :] = weight
        den = jnp.sum(weight.astype(F32), axis=1, keepdims=True)
        tops = jnp.where(head_of == h, top, tops)
        dens = jnp.where(head_of == h, den, dens)
    for p in range(n_src):
        send_stat[p, :, :channels] = tops[p * own : (p + 1) * own]
        send_stat[p, :, channels:] = dens[p * own : (p + 1) * own]
    relay(1)
    sums_of(0)
    for j in range(1, n_src):
        copy = stat_copy(j, s)
        copy.start()
        started.append(copy)
    send_sums(0)
    collect(1)
    spread(1)
    relay(2)
    loads[1].wait()
    loads[2].wait()
    sums_of(1)
    send_sums(1)
    collect(2)
    spread(2)
    loads[3].wait()
    loads[4].wait()
    sums_of(2)
    send_sums(2)

    for j in range(1, n_src):
        stat_copy(j, other(j)).wait_recv()
    stats = [send_stat[s]] + [recv_stat[other(j)] for j in range(1, n_src)]
    top = functools.reduce(jnp.maximum, [a[:, :channels] for a in stats])
    scales = [jnp.exp(a[:, :channels] - top) for a in stats]
    den = sum(a[:, channels:] * b for a, b in zip(stats, scales))
    inverse = 1.0 / den
    scales = [a * inverse for a in scales]
    loads[5].wait()
    for k, (first, count) in enumerate(PIECES):
        for j in range(1, n_src):
            num_copy(j, k, other(j)).wait_recv()
        for i in range(first, first + count):
            columns = pl.ds(i * channels, channels)
            total = send_num[s, :, columns].astype(F32) * scales[0]
            for j in range(1, n_src):
                total += recv_num[other(j), :, columns].astype(F32) * scales[j]
            merged_ref[i] = total
    for degree in range(w_out_hbm.shape[0]):
        members = [i for i, l in enumerate(DEGREES) if l == degree]
        stacked = jnp.concatenate([merged_ref[i] for i in members], axis=0).astype(BF16)
        result = dot(stacked, w_out[degree])
        for at, i in enumerate(members):
            out_ref[:, i * channels : (i + 1) * channels] = result[at * own : (at + 1) * own].astype(BF16)

    for copy in started:
        copy.wait_send()


def solution(mesh):
    n_dst, n_src = mesh.shape["dst"], mesh.shape["src"]

    def shards(
        features,
        edge_source,
        edge_target,
        edge_valid,
        edge_radial,
        edge_bias,
        w_radial,
        w_zero,
        w_one_re,
        w_one_im,
        w_two_re,
        w_two_im,
        att_vector,
        w_out,
    ):
        own, width = features.shape
        slots = edge_source.shape[1]
        channels = w_radial.shape[1]
        block = own * n_src
        atoms = own * n_dst
        pieces = len(PIECES)
        weights = (w_zero, w_one_re, w_one_im, w_two_re, w_two_im, w_out)
        vmem = pl.BlockSpec(memory_space=pltpu.VMEM)
        hbm = pl.BlockSpec(memory_space=pl.ANY)
        return pl.pallas_call(
            functools.partial(kernel, n_dst, n_src),
            out_shape=jax.ShapeDtypeStruct((own, width), BF16),
            in_specs=[vmem] * 8 + [hbm] * 6,
            out_specs=vmem,
            scratch_shapes=[pltpu.VMEM(w.shape, w.dtype) for w in weights]
            + [
                pltpu.VMEM((n_dst, own, width), BF16),
                pltpu.VMEM((atoms, width), F32),
                pltpu.VMEM((slots, channels), F32),
                pltpu.VMEM((slots, atoms), BF16),
                pltpu.VMEM((slots, width), BF16),
                pltpu.VMEM((HEADS * block, slots), BF16),
                pltpu.VMEM((block, width), F32),
                pltpu.VMEM((n_src, own, width), BF16),
                pltpu.VMEM((n_src, own, width), BF16),
                pltpu.VMEM((n_src, own, 2 * channels), F32),
                pltpu.VMEM((n_src, own, 2 * channels), F32),
                pltpu.VMEM((width // channels, own, channels), F32),
                pltpu.SemaphoreType.DMA((len(weights),)),
                pltpu.SemaphoreType.DMA((n_dst // CORES, pieces)),
                pltpu.SemaphoreType.DMA((n_dst // CORES, pieces)),
                pltpu.SemaphoreType.DMA((n_dst, pieces)),
                pltpu.SemaphoreType.DMA((n_src, pieces + 1)),
                pltpu.SemaphoreType.DMA((n_src, pieces + 1)),
            ],
            compiler_params=pltpu.CompilerParams(
                collective_id=0,
                has_side_effects=True,
                vmem_limit_bytes=60 * 1024 * 1024,
            ),
        )(
            features,
            edge_source,
            edge_target,
            edge_valid,
            edge_radial,
            edge_bias,
            w_radial,
            att_vector.reshape(1, channels),
            *weights,
        )

    in_specs = (
        P(("dst", "src"), None),
        P("dst", "src"),
        P("dst", "src"),
        P("dst", "src"),
        P("dst", "src", None),
        P("dst", None, "src"),
        P(),
        P(),
        P(),
        P(),
        P(),
        P(),
        P(),
        P(),
    )
    out_specs = P(("dst", "src"), None)
    return jax.shard_map(shards, mesh=mesh, in_specs=in_specs, out_specs=out_specs, check_vma=False)
```

```python
import functools

import jax
import jax.numpy as jnp
from jax import lax
from jax.experimental import pallas as pl
from jax.experimental.pallas import tpu as pltpu
from jax.sharding import PartitionSpec as P

HEADS = 8
NEG = -1e30
MESH = pl.DeviceIdType.MESH
CORES = 2
PIECES = ((0, 7), (7, 12), (19, 10))
DEGREES = list(range(7)) + list(range(1, 7)) * 2 + list(range(2, 7)) * 2
F32 = jnp.float32
BF16 = jnp.bfloat16


def dot(left, right):
    return jnp.dot(left, right, preferred_element_type=F32)


def kernel(
    n_dst,
    n_src,
    feat_hbm,
    source_hbm,
    target_hbm,
    valid_hbm,
    radial_hbm,
    bias_hbm,
    w_radial_hbm,
    att_hbm,
    w_zero_hbm,
    w_one_re_hbm,
    w_one_im_hbm,
    w_two_re_hbm,
    w_two_im_hbm,
    w_out_hbm,
    out_ref,
    feat_ref,
    source_ref,
    target_ref,
    valid_ref,
    radial_ref,
    bias_ref,
    w_radial_ref,
    att_ref,
    w_zero,
    w_one_re,
    w_one_im,
    w_two_re,
    w_two_im,
    w_out,
    feat_buf,
    feat_all,
    gain_ref,
    onehot_ref,
    u_ref,
    weight_ref,
    num_ref,
    send_num,
    recv_num,
    send_stat,
    recv_stat,
    input_sem,
    load_sem,
    z_send,
    pair_send,
    feat_recv,
    num_send,
    num_recv,
):
    own = feat_ref.shape[0]
    channels = w_radial_ref.shape[1]
    slots = source_ref.shape[1]
    block = own * n_src
    atoms = own * n_dst
    nz = n_dst // CORES
    per_head = channels // HEADS
    d = lax.axis_index("dst")
    s = lax.axis_index("src")
    z = d // CORES
    core = d % CORES
    partner = d + 1 - 2 * core

    def line(j):
        return lax.rem(z + j, nz) * CORES + core

    def other(j):
        return lax.rem(s + j, n_src)

    fetches = [
        pltpu.make_async_copy(src, dst, input_sem.at[i])
        for i, (src, dst) in enumerate(
            (
                (feat_hbm, feat_ref),
                (radial_hbm, radial_ref),
                (w_radial_hbm, w_radial_ref),
                (source_hbm, source_ref),
                (target_hbm, target_ref),
                (valid_hbm, valid_ref),
                (bias_hbm, bias_ref),
                (att_hbm, att_ref),
            )
        )
    ]
    for fetch in fetches:
        fetch.start()

    barrier = pltpu.get_barrier_semaphore()
    for j in range(1, nz):
        pl.semaphore_signal(barrier, inc=1, device_id=(line(j), s), device_id_type=MESH)
    for j in range(1, n_src):
        pl.semaphore_signal(barrier, inc=1, device_id=(d, other(j)), device_id_type=MESH)
    pl.semaphore_signal(barrier, inc=1, device_id=(partner, s), device_id_type=MESH)

    loads = [
        pltpu.make_async_copy(src, dst, load_sem.at[i])
        for i, (src, dst) in enumerate(
            (
                (w_zero_hbm, w_zero),
                (w_one_re_hbm, w_one_re),
                (w_one_im_hbm, w_one_im),
                (w_two_re_hbm, w_two_re),
                (w_two_im_hbm, w_two_im),
                (w_out_hbm, w_out),
            )
        )
    ]
    for load in loads:
        load.start()

    def span(k):
        first, count = PIECES[k]
        return pl.ds(first * channels, count * channels)

    def feature_copy(k, src, index, send, target):
        return pltpu.make_async_remote_copy(
            src_ref=src,
            dst_ref=feat_buf.at[index, :, span(k)],
            send_sem=send,
            recv_sem=feat_recv.at[index, k],
            device_id=(target, s),
            device_id_type=MESH,
        )

    fetches[0].wait()
    pl.semaphore_wait(barrier, nz - 1 + n_src - 1 + 1)

    started = []
    for k in range(len(PIECES)):
        mine = feat_ref.at[:, span(k)]
        for j in range(1, nz):
            copy = feature_copy(k, mine, d, z_send.at[j, k], line(j))
            copy.start()
            started.append(copy)
        copy = feature_copy(k, mine, d, pair_send.at[0, k], partner)
        copy.start()
        started.append(copy)

    for fetch in fetches[1:]:
        fetch.wait()
    gain_ref[...] = dot(radial_ref[0], w_radial_ref[...])
    source = source_ref[...]
    row = source // block * own + source % own
    picks = lax.broadcasted_iota(jnp.int32, (atoms, slots), 0) == row
    onehot_ref[...] = jnp.transpose(picks.astype(F32)).astype(BF16)

    def relay(k):
        for j in range(1, nz):
            index = line(j)
            feature_copy(k, feat_buf.at[index, :, span(k)], index, z_send.at[j, k], index).wait_recv()
            copy = feature_copy(k, feat_buf.at[index, :, span(k)], index, pair_send.at[j, k], partner)
            copy.start()
            started.append(copy)

    def collect(k):
        mine = pl.ds(pl.multiple_of(d * own, own), own)
        feat_all[mine, span(k)] = feat_ref[:, span(k)].astype(F32)
        for j in range(1, nz):
            index = line(j)
            rows = pl.ds(pl.multiple_of(index * own, own), own)
            feat_all[rows, span(k)] = feat_buf[index, :, span(k)].astype(F32)
        for j in range(nz):
            index = lax.rem(z + j, nz) * CORES + 1 - core
            feature_copy(k, feat_buf.at[index, :, span(k)], index, pair_send.at[j, k], partner).wait_recv()
            rows = pl.ds(pl.multiple_of(index * own, own), own)
            feat_all[rows, span(k)] = feat_buf[index, :, span(k)].astype(F32)

    def spread(k):
        first, count = PIECES[k]
        rows = dot(onehot_ref[...], feat_all[:, span(k)].astype(BF16))
        gain = gain_ref[...]
        for i in range(count):
            at = (first + i) * channels
            u_ref[:, at : at + channels] = (rows[:, i * channels : (i + 1) * channels] * gain).astype(BF16)

    head_of = lax.broadcasted_iota(jnp.int32, (1, channels), 1) // per_head
    together = max(1, 256 // block)
    groups = HEADS // together

    def gather_sums(k, group):
        first, count = PIECES[k]
        rows = pl.ds(group * (together * block), together * block)
        weights = weight_ref[rows, :]
        sums = dot(weights, u_ref[:, span(k)]).astype(BF16)
        if k == 0:
            parts = [dot(sums, w_zero[...])]
        else:
            w_re, w_im = ((w_one_re, w_one_im), (w_two_re, w_two_im))[k - 1]
            half = count // 2 * channels
            plus, minus = sums[:, :half], sums[:, half:]
            parts = [
                dot(plus, w_re[...]) - dot(minus, w_im[...]),
                dot(plus, w_im[...]) + dot(minus, w_re[...]),
            ]
        at = first
        for part in parts:
            for i in range(part.shape[1] // channels):
                columns = pl.ds(at * channels, channels)
                at += 1
                value = part[:, i * channels : (i + 1) * channels]
                total = num_ref[:, columns] if groups > 1 else jnp.zeros((block, channels), F32)
                for j in range(together):
                    head = group * together + j
                    total = jnp.where(head_of == head, value[j * block : (j + 1) * block], total)
                num_ref[:, columns] = total

    def sums_of(k):
        if groups == 1:
            gather_sums(k, 0)
        else:
            lax.fori_loop(0, groups, lambda g, c: (gather_sums(k, g), c)[1], 0)
        first, count = PIECES[k]
        for p in range(n_src):
            send_num[p, :, span(k)] = num_ref[p * own : (p + 1) * own, span(k)].astype(BF16)

    def stat_copy(j, source_at):
        return pltpu.make_async_remote_copy(
            src_ref=send_stat.at[other(j)],
            dst_ref=recv_stat.at[source_at],
            send_sem=num_send.at[j, len(PIECES)],
            recv_sem=num_recv.at[source_at, len(PIECES)],
            device_id=(d, other(j)),
            device_id_type=MESH,
        )

    def num_copy(j, k, source_at):
        return pltpu.make_async_remote_copy(
            src_ref=send_num.at[other(j), :, span(k)],
            dst_ref=recv_num.at[source_at, :, span(k)],
            send_sem=num_send.at[j, k],
            recv_sem=num_recv.at[source_at, k],
            device_id=(d, other(j)),
            device_id_type=MESH,
        )

    def send_sums(k):
        for j in range(1, n_src):
            copy = num_copy(j, k, s)
            copy.start()
            started.append(copy)

    relay(0)
    collect(0)
    spread(0)
    loads[0].wait()
    scalar = dot(u_ref[:, span(0)], w_zero[:, :channels])
    active = scalar / (1.0 + jnp.exp(-scalar))
    att = jnp.where(
        lax.broadcasted_iota(jnp.int32, (HEADS, channels), 0) == head_of, att_ref[...], 0.0
    )
    logit = lax.dot_general(
        att,
        active,
        (((1,), (1,)), ((), ())),
        precision=lax.Precision.HIGHEST,
        preferred_element_type=F32,
    ) + bias_ref[0]
    local_target = target_ref[...] - d * block
    member = (lax.broadcasted_iota(jnp.int32, (block, slots), 0) == local_target) & (valid_ref[...] > 0)
    tops = jnp.zeros((block, channels), F32)
    dens = jnp.zeros((block, channels), F32)
    for h in range(HEADS):
        masked = jnp.where(member, logit[h : h + 1, :], NEG)
        top = jnp.max(masked, axis=1, keepdims=True)
        weight = jnp.where(member, jnp.exp(masked - top), 0.0).astype(BF16)
        weight_ref[h * block : (h + 1) * block, :] = weight
        den = jnp.sum(weight.astype(F32), axis=1, keepdims=True)
        tops = jnp.where(head_of == h, top, tops)
        dens = jnp.where(head_of == h, den, dens)
    for p in range(n_src):
        send_stat[p, :, :channels] = tops[p * own : (p + 1) * own]
        send_stat[p, :, channels:] = dens[p * own : (p + 1) * own]
    relay(1)
    sums_of(0)
    for j in range(1, n_src):
        copy = stat_copy(j, s)
        copy.start()
        started.append(copy)
    send_sums(0)
    collect(1)
    spread(1)
    relay(2)
    loads[1].wait()
    loads[2].wait()
    sums_of(1)
    send_sums(1)
    collect(2)
    spread(2)
    loads[3].wait()
    loads[4].wait()
    sums_of(2)
    send_sums(2)

    for j in range(1, n_src):
        stat_copy(j, other(j)).wait_recv()
    stats = [send_stat[s]] + [recv_stat[other(j)] for j in range(1, n_src)]
    top = functools.reduce(jnp.maximum, [a[:, :channels] for a in stats])
    scales = [jnp.exp(a[:, :channels] - top) for a in stats]
    den = sum(a[:, channels:] * b for a, b in zip(stats, scales))
    inverse = 1.0 / den
    scales = [a * inverse for a in scales]
    loads[5].wait()
    for k, (first, count) in enumerate(PIECES):
        for j in range(1, n_src):
            num_copy(j, k, other(j)).wait_recv()
        for degree in sorted(set(DEGREES[first : first + count])):
            members = [i for i in range(first, first + count) if DEGREES[i] == degree]
            merged = []
            for i in members:
                columns = pl.ds(i * channels, channels)
                total = send_num[s, :, columns].astype(F32) * scales[0]
                for j in range(1, n_src):
                    total += recv_num[other(j), :, columns].astype(F32) * scales[j]
                merged.append(total)
            result = dot(jnp.concatenate(merged, axis=0).astype(BF16), w_out[degree])
            for at, i in enumerate(members):
                out_ref[:, i * channels : (i + 1) * channels] = result[at * own : (at + 1) * own].astype(BF16)

    for copy in started:
        copy.wait_send()


def solution(mesh):
    n_dst, n_src = mesh.shape["dst"], mesh.shape["src"]

    def shards(
        features,
        edge_source,
        edge_target,
        edge_valid,
        edge_radial,
        edge_bias,
        w_radial,
        w_zero,
        w_one_re,
        w_one_im,
        w_two_re,
        w_two_im,
        att_vector,
        w_out,
    ):
        own, width = features.shape
        slots = edge_source.shape[1]
        channels = w_radial.shape[1]
        block = own * n_src
        atoms = own * n_dst
        pieces = len(PIECES)
        weights = (w_zero, w_one_re, w_one_im, w_two_re, w_two_im, w_out)
        operands = (
            features,
            edge_source,
            edge_target,
            edge_valid,
            edge_radial,
            edge_bias,
            w_radial,
            att_vector.reshape(1, channels),
            *weights,
        )
        vmem = pl.BlockSpec(memory_space=pltpu.VMEM)
        hbm = pl.BlockSpec(memory_space=pl.ANY)
        return pl.pallas_call(
            functools.partial(kernel, n_dst, n_src),
            out_shape=jax.ShapeDtypeStruct((own, width), BF16),
            in_specs=[hbm] * len(operands),
            out_specs=vmem,
            scratch_shapes=[pltpu.VMEM(w.shape, w.dtype) for w in operands]
            + [
                pltpu.VMEM((n_dst, own, width), BF16),
                pltpu.VMEM((atoms, width), F32),
                pltpu.VMEM((slots, channels), F32),
                pltpu.VMEM((slots, atoms), BF16),
                pltpu.VMEM((slots, width), BF16),
                pltpu.VMEM((HEADS * block, slots), BF16),
                pltpu.VMEM((block, width), F32),
                pltpu.VMEM((n_src, own, width), BF16),
                pltpu.VMEM((n_src, own, width), BF16),
                pltpu.VMEM((n_src, own, 2 * channels), F32),
                pltpu.VMEM((n_src, own, 2 * channels), F32),
                pltpu.SemaphoreType.DMA((len(operands) - len(weights),)),
                pltpu.SemaphoreType.DMA((len(weights),)),
                pltpu.SemaphoreType.DMA((n_dst // CORES, pieces)),
                pltpu.SemaphoreType.DMA((n_dst // CORES, pieces)),
                pltpu.SemaphoreType.DMA((n_dst, pieces)),
                pltpu.SemaphoreType.DMA((n_src, pieces + 1)),
                pltpu.SemaphoreType.DMA((n_src, pieces + 1)),
            ],
            compiler_params=pltpu.CompilerParams(
                collective_id=0,
                has_side_effects=True,
                vmem_limit_bytes=60 * 1024 * 1024,
            ),
        )(*operands)

    in_specs = (
        P(("dst", "src"), None),
        P("dst", "src"),
        P("dst", "src"),
        P("dst", "src"),
        P("dst", "src", None),
        P("dst", None, "src"),
        P(),
        P(),
        P(),
        P(),
        P(),
        P(),
        P(),
        P(),
    )
    out_specs = P(("dst", "src"), None)
    return jax.shard_map(shards, mesh=mesh, in_specs=in_specs, out_specs=out_specs, check_vma=False)
```

```python
import functools

import jax
import jax.numpy as jnp
from jax import lax
from jax.experimental import pallas as pl
from jax.experimental.pallas import tpu as pltpu
from jax.sharding import PartitionSpec as P

HEADS = 8
NEG = -1e30
MESH = pl.DeviceIdType.MESH
CORES = 2
PIECES = ((0, 7), (7, 12), (19, 10))
DEGREES = list(range(7)) + list(range(1, 7)) * 2 + list(range(2, 7)) * 2
F32 = jnp.float32
BF16 = jnp.bfloat16


def dot(left, right):
    return jnp.dot(left, right, preferred_element_type=F32)


def kernel(
    n_dst,
    n_src,
    feat_hbm,
    source_hbm,
    target_hbm,
    valid_hbm,
    radial_hbm,
    bias_hbm,
    w_radial_hbm,
    att_hbm,
    w_zero_hbm,
    w_one_re_hbm,
    w_one_im_hbm,
    w_two_re_hbm,
    w_two_im_hbm,
    w_out_hbm,
    out_ref,
    feat_ref,
    source_ref,
    target_ref,
    valid_ref,
    radial_ref,
    bias_ref,
    w_radial_ref,
    att_ref,
    w_zero,
    w_one_re,
    w_one_im,
    w_two_re,
    w_two_im,
    w_out,
    feat_buf,
    feat_all,
    gain_ref,
    onehot_ref,
    u_ref,
    weight_ref,
    num_ref,
    send_num,
    recv_num,
    send_stat,
    recv_stat,
    input_sem,
    load_sem,
    z_send,
    pair_send,
    feat_recv,
    num_send,
    num_recv,
):
    own = feat_ref.shape[0]
    channels = w_radial_ref.shape[1]
    slots = source_ref.shape[1]
    block = own * n_src
    atoms = own * n_dst
    nz = n_dst // CORES
    per_head = channels // HEADS
    d = lax.axis_index("dst")
    s = lax.axis_index("src")
    z = d // CORES
    core = d % CORES
    partner = d + 1 - 2 * core

    def line(j):
        return lax.rem(z + j, nz) * CORES + core

    def other(j):
        return lax.rem(s + j, n_src)

    fetches = [
        pltpu.make_async_copy(src, dst, input_sem.at[i])
        for i, (src, dst) in enumerate(
            (
                (feat_hbm, feat_ref),
                (radial_hbm, radial_ref),
                (w_radial_hbm, w_radial_ref),
                (source_hbm, source_ref),
                (target_hbm, target_ref),
                (valid_hbm, valid_ref),
                (bias_hbm, bias_ref),
                (att_hbm, att_ref),
            )
        )
    ]
    for fetch in fetches:
        fetch.start()

    barrier = pltpu.get_barrier_semaphore()
    for j in range(1, nz):
        pl.semaphore_signal(barrier, inc=1, device_id=(line(j), s), device_id_type=MESH)
    for j in range(1, n_src):
        pl.semaphore_signal(barrier, inc=1, device_id=(d, other(j)), device_id_type=MESH)
    pl.semaphore_signal(barrier, inc=1, device_id=(partner, s), device_id_type=MESH)

    loads = [
        pltpu.make_async_copy(src, dst, load_sem.at[i])
        for i, (src, dst) in enumerate(
            (
                (w_zero_hbm, w_zero),
                (w_one_re_hbm, w_one_re),
                (w_one_im_hbm, w_one_im),
                (w_two_re_hbm, w_two_re),
                (w_two_im_hbm, w_two_im),
                (w_out_hbm, w_out),
            )
        )
    ]
    for load in loads:
        load.start()

    def span(k):
        first, count = PIECES[k]
        return pl.ds(first * channels, count * channels)

    def feature_copy(k, src, index, send, target):
        return pltpu.make_async_remote_copy(
            src_ref=src,
            dst_ref=feat_buf.at[index, :, span(k)],
            send_sem=send,
            recv_sem=feat_recv.at[index, k],
            device_id=(target, s),
            device_id_type=MESH,
        )

    fetches[0].wait()
    pl.semaphore_wait(barrier, nz - 1 + n_src - 1 + 1)

    started = []

    def offer(k):
        mine = feat_ref.at[:, span(k)]
        for j in range(1, nz):
            copy = feature_copy(k, mine, d, z_send.at[j, k], line(j))
            copy.start()
            started.append(copy)
        copy = feature_copy(k, mine, d, pair_send.at[0, k], partner)
        copy.start()
        started.append(copy)

    offer(0)

    for fetch in fetches[1:]:
        fetch.wait()
    gain_ref[...] = dot(radial_ref[0], w_radial_ref[...])
    source = source_ref[...]
    row = source // block * own + source % own
    picks = lax.broadcasted_iota(jnp.int32, (atoms, slots), 0) == row
    onehot_ref[...] = jnp.transpose(picks.astype(F32)).astype(BF16)

    def relay(k):
        for j in range(1, nz):
            index = line(j)
            feature_copy(k, feat_buf.at[index, :, span(k)], index, z_send.at[j, k], index).wait_recv()
            copy = feature_copy(k, feat_buf.at[index, :, span(k)], index, pair_send.at[j, k], partner)
            copy.start()
            started.append(copy)

    def collect(k):
        mine = pl.ds(pl.multiple_of(d * own, own), own)
        feat_all[mine, span(k)] = feat_ref[:, span(k)].astype(F32)
        for j in range(1, nz):
            index = line(j)
            rows = pl.ds(pl.multiple_of(index * own, own), own)
            feat_all[rows, span(k)] = feat_buf[index, :, span(k)].astype(F32)
        for j in range(nz):
            index = lax.rem(z + j, nz) * CORES + 1 - core
            feature_copy(k, feat_buf.at[index, :, span(k)], index, pair_send.at[j, k], partner).wait_recv()
            rows = pl.ds(pl.multiple_of(index * own, own), own)
            feat_all[rows, span(k)] = feat_buf[index, :, span(k)].astype(F32)

    def spread(k):
        first, count = PIECES[k]
        rows = dot(onehot_ref[...], feat_all[:, span(k)].astype(BF16))
        gain = gain_ref[...]
        for i in range(count):
            at = (first + i) * channels
            u_ref[:, at : at + channels] = (rows[:, i * channels : (i + 1) * channels] * gain).astype(BF16)

    head_of = lax.broadcasted_iota(jnp.int32, (1, channels), 1) // per_head
    together = max(1, 256 // block)
    groups = HEADS // together

    def gather_sums(k, group):
        first, count = PIECES[k]
        rows = pl.ds(group * (together * block), together * block)
        weights = weight_ref[rows, :]
        sums = dot(weights, u_ref[:, span(k)]).astype(BF16)
        if k == 0:
            parts = [dot(sums, w_zero[...])]
        else:
            w_re, w_im = ((w_one_re, w_one_im), (w_two_re, w_two_im))[k - 1]
            half = count // 2 * channels
            plus, minus = sums[:, :half], sums[:, half:]
            parts = [
                dot(plus, w_re[...]) - dot(minus, w_im[...]),
                dot(plus, w_im[...]) + dot(minus, w_re[...]),
            ]
        at = first
        for part in parts:
            for i in range(part.shape[1] // channels):
                columns = pl.ds(at * channels, channels)
                at += 1
                value = part[:, i * channels : (i + 1) * channels]
                total = num_ref[:, columns] if groups > 1 else jnp.zeros((block, channels), F32)
                for j in range(together):
                    head = group * together + j
                    total = jnp.where(head_of == head, value[j * block : (j + 1) * block], total)
                num_ref[:, columns] = total

    def sums_of(k):
        if groups == 1:
            gather_sums(k, 0)
        else:
            lax.fori_loop(0, groups, lambda g, c: (gather_sums(k, g), c)[1], 0)
        first, count = PIECES[k]
        for p in range(n_src):
            send_num[p, :, span(k)] = num_ref[p * own : (p + 1) * own, span(k)].astype(BF16)

    def stat_copy(j, source_at):
        return pltpu.make_async_remote_copy(
            src_ref=send_stat.at[other(j)],
            dst_ref=recv_stat.at[source_at],
            send_sem=num_send.at[j, len(PIECES)],
            recv_sem=num_recv.at[source_at, len(PIECES)],
            device_id=(d, other(j)),
            device_id_type=MESH,
        )

    def num_copy(j, k, source_at):
        return pltpu.make_async_remote_copy(
            src_ref=send_num.at[other(j), :, span(k)],
            dst_ref=recv_num.at[source_at, :, span(k)],
            send_sem=num_send.at[j, k],
            recv_sem=num_recv.at[source_at, k],
            device_id=(d, other(j)),
            device_id_type=MESH,
        )

    def send_sums(k):
        for j in range(1, n_src):
            copy = num_copy(j, k, s)
            copy.start()
            started.append(copy)

    relay(0)
    offer(1)
    offer(2)
    collect(0)
    spread(0)
    loads[0].wait()
    scalar = dot(u_ref[:, span(0)], w_zero[:, :channels])
    active = scalar / (1.0 + jnp.exp(-scalar))
    att = jnp.where(
        lax.broadcasted_iota(jnp.int32, (HEADS, channels), 0) == head_of, att_ref[...], 0.0
    )
    logit = lax.dot_general(
        att,
        active,
        (((1,), (1,)), ((), ())),
        precision=lax.Precision.HIGHEST,
        preferred_element_type=F32,
    ) + bias_ref[0]
    local_target = target_ref[...] - d * block
    member = (lax.broadcasted_iota(jnp.int32, (block, slots), 0) == local_target) & (valid_ref[...] > 0)
    tops = jnp.zeros((block, channels), F32)
    dens = jnp.zeros((block, channels), F32)
    for h in range(HEADS):
        masked = jnp.where(member, logit[h : h + 1, :], NEG)
        top = jnp.max(masked, axis=1, keepdims=True)
        weight = jnp.where(member, jnp.exp(masked - top), 0.0).astype(BF16)
        weight_ref[h * block : (h + 1) * block, :] = weight
        den = jnp.sum(weight.astype(F32), axis=1, keepdims=True)
        tops = jnp.where(head_of == h, top, tops)
        dens = jnp.where(head_of == h, den, dens)
    for p in range(n_src):
        send_stat[p, :, :channels] = tops[p * own : (p + 1) * own]
        send_stat[p, :, channels:] = dens[p * own : (p + 1) * own]
    relay(1)
    for j in range(1, n_src):
        copy = stat_copy(j, s)
        copy.start()
        started.append(copy)
    sums_of(0)
    send_sums(0)
    collect(1)
    spread(1)
    relay(2)
    loads[1].wait()
    loads[2].wait()
    sums_of(1)
    send_sums(1)
    collect(2)
    spread(2)
    loads[3].wait()
    loads[4].wait()
    sums_of(2)
    send_sums(2)

    for j in range(1, n_src):
        stat_copy(j, other(j)).wait_recv()
    stats = [send_stat[s]] + [recv_stat[other(j)] for j in range(1, n_src)]
    top = functools.reduce(jnp.maximum, [a[:, :channels] for a in stats])
    scales = [jnp.exp(a[:, :channels] - top) for a in stats]
    den = sum(a[:, channels:] * b for a, b in zip(stats, scales))
    inverse = 1.0 / den
    scales = [a * inverse for a in scales]
    loads[5].wait()
    for k, (first, count) in enumerate(PIECES):
        for j in range(1, n_src):
            num_copy(j, k, other(j)).wait_recv()
        for degree in sorted(set(DEGREES[first : first + count])):
            members = [i for i in range(first, first + count) if DEGREES[i] == degree]
            merged = []
            for i in members:
                columns = pl.ds(i * channels, channels)
                total = send_num[s, :, columns].astype(F32) * scales[0]
                for j in range(1, n_src):
                    total += recv_num[other(j), :, columns].astype(F32) * scales[j]
                merged.append(total)
            result = dot(jnp.concatenate(merged, axis=0).astype(BF16), w_out[degree])
            for at, i in enumerate(members):
                out_ref[:, i * channels : (i + 1) * channels] = result[at * own : (at + 1) * own].astype(BF16)

    for copy in started:
        copy.wait_send()


def solution(mesh):
    n_dst, n_src = mesh.shape["dst"], mesh.shape["src"]

    def shards(
        features,
        edge_source,
        edge_target,
        edge_valid,
        edge_radial,
        edge_bias,
        w_radial,
        w_zero,
        w_one_re,
        w_one_im,
        w_two_re,
        w_two_im,
        att_vector,
        w_out,
    ):
        own, width = features.shape
        slots = edge_source.shape[1]
        channels = w_radial.shape[1]
        block = own * n_src
        atoms = own * n_dst
        pieces = len(PIECES)
        weights = (w_zero, w_one_re, w_one_im, w_two_re, w_two_im, w_out)
        operands = (
            features,
            edge_source,
            edge_target,
            edge_valid,
            edge_radial,
            edge_bias,
            w_radial,
            att_vector.reshape(1, channels),
            *weights,
        )
        vmem = pl.BlockSpec(memory_space=pltpu.VMEM)
        hbm = pl.BlockSpec(memory_space=pl.ANY)
        return pl.pallas_call(
            functools.partial(kernel, n_dst, n_src),
            out_shape=jax.ShapeDtypeStruct((own, width), BF16),
            in_specs=[hbm] * len(operands),
            out_specs=vmem,
            scratch_shapes=[pltpu.VMEM(w.shape, w.dtype) for w in operands]
            + [
                pltpu.VMEM((n_dst, own, width), BF16),
                pltpu.VMEM((atoms, width), F32),
                pltpu.VMEM((slots, channels), F32),
                pltpu.VMEM((slots, atoms), BF16),
                pltpu.VMEM((slots, width), BF16),
                pltpu.VMEM((HEADS * block, slots), BF16),
                pltpu.VMEM((block, width), F32),
                pltpu.VMEM((n_src, own, width), BF16),
                pltpu.VMEM((n_src, own, width), BF16),
                pltpu.VMEM((n_src, own, 2 * channels), F32),
                pltpu.VMEM((n_src, own, 2 * channels), F32),
                pltpu.SemaphoreType.DMA((len(operands) - len(weights),)),
                pltpu.SemaphoreType.DMA((len(weights),)),
                pltpu.SemaphoreType.DMA((n_dst // CORES, pieces)),
                pltpu.SemaphoreType.DMA((n_dst // CORES, pieces)),
                pltpu.SemaphoreType.DMA((n_dst, pieces)),
                pltpu.SemaphoreType.DMA((n_src, pieces + 1)),
                pltpu.SemaphoreType.DMA((n_src, pieces + 1)),
            ],
            compiler_params=pltpu.CompilerParams(
                collective_id=0,
                has_side_effects=True,
                vmem_limit_bytes=60 * 1024 * 1024,
            ),
        )(*operands)

    in_specs = (
        P(("dst", "src"), None),
        P("dst", "src"),
        P("dst", "src"),
        P("dst", "src"),
        P("dst", "src", None),
        P("dst", None, "src"),
        P(),
        P(),
        P(),
        P(),
        P(),
        P(),
        P(),
        P(),
    )
    out_specs = P(("dst", "src"), None)
    return jax.shard_map(shards, mesh=mesh, in_specs=in_specs, out_specs=out_specs, check_vma=False)
```
